32 devices in a mesh: tm: 8 (over y, x, core), chan: 4 (over z).
Axes of the slice: x: 2, y: 2, z: 4, core: 2. Of those that a mesh axis runs over, the one named last changes fastest.
Arguments:
- inputs: bfloat16 [4096, 8192], P('tm', 'chan'), may hold values from -52 to 52
- gate_logits: bfloat16 [4096, 8192], P(('tm', 'chan')), may hold values from -5 to 5
- step_sizes: bfloat16 [4096, 64], P('tm', 'chan'), may hold values from 0.3 to 28672, as said below
- decay_rates: float32 [8192], replicated, as said below
- skip_gain: float32 [8192], replicated, may hold values from 0.3 to 0.8
- norm_gain: float32 [8192], replicated, may hold values from 0.25 to 1.75
Outputs:
- outputs: bfloat16 [4096, 8192], P(('tm', 'chan'))
The draws below stay inside these ranges and needn't reach their ends.
Inputs may be any that keep to these rules, and one draw needn't show every extreme that they name: `step_sizes`: every step size is positive. `decay_rates`: every rate is positive.
All inputs are finite; a program needn't handle non-finite values.
Results may differ from the reference program's by a relative error of at most 0.0049.
Values may be sent and summed in bfloat16 or wider, within the bound.
A program may use at most 64 MiB of HBM per device.

```python
import math
import jax
import jax.numpy as jnp
from jax import lax

N = 8192
HEAD_SIZE = 128
HEADS = 64
TOK_DEV = 512
TOKENS = 4096


def head_profile(key):
    anchor = jax.random.fold_in(key, 7103)
    ranking = jax.random.permutation(jax.random.fold_in(anchor, 1), HEADS)
    fast_count = HEADS // 2
    is_fast = ranking < fast_count
    fast_low = math.log(0.75 / TOK_DEV)
    fast_high = math.log(1.0 / 25.0)
    jitter = jax.random.uniform(jax.random.fold_in(anchor, 2), (HEADS,), jnp.float32, 0.0, 1.0)
    place = (ranking.astype(jnp.float32) + jitter) / float(fast_count)
    place = jnp.clip(place, 0.0, 1.0)
    fast_rate = jnp.exp(fast_low + place * (fast_high - fast_low))
    slow_rate = jnp.exp(jax.random.uniform(jax.random.fold_in(anchor, 3), (HEADS,), jnp.float32, math.log(1.3), math.log(1.8))) / TOKENS
    return jnp.where(is_fast, fast_rate, slow_rate)


def draw_decay_rates(key, part):
    head_rate = head_profile(key)
    factor = jnp.exp(jax.random.uniform(jax.random.fold_in(key, 11), (N,), jnp.float32, math.log(0.7), math.log(1.45)))
    return (jnp.repeat(head_rate, HEAD_SIZE) * factor).astype(jnp.float32)


def draw_step_sizes(key, part):
    head_rate = head_profile(key)
    anchor = jax.random.fold_in(key, 29)
    block_count = TOKENS // TOK_DEV
    device_factor = jnp.exp(jax.random.uniform(jax.random.fold_in(anchor, 1), (block_count,), jnp.float32, math.log(0.6), math.log(1.6)))
    token_factor = jnp.exp(jax.random.uniform(jax.random.fold_in(anchor, 2), (TOKENS, HEADS), jnp.float32, math.log(0.7), math.log(1.4)))
    sizes_now = jnp.repeat(device_factor, TOK_DEV)[:, None] * token_factor
    places = jax.random.randint(jax.random.fold_in(anchor, 3), (2, HEADS), 0, TOKENS)
    strength = jnp.exp(jax.random.uniform(jax.random.fold_in(anchor, 4), (2, HEADS), jnp.float32, math.log(0.22), math.log(0.5)))
    positions = jnp.arange(TOKENS, dtype=jnp.int32)[:, None]
    first_hit = positions == places[0][None, :]
    sizes_now = jnp.where(first_hit, (strength[0] / head_rate)[None, :], sizes_now)
    second_hit = positions == places[1][None, :]
    sizes_now = jnp.where(second_hit, (strength[1] / head_rate)[None, :], sizes_now)
    return sizes_now.astype(jnp.bfloat16)


def draw_inputs(key, part):
    anchor = jax.random.fold_in(key, 53)
    noise = jnp.clip(jax.random.normal(jax.random.fold_in(anchor, 1), (TOKENS, N), jnp.float32), -4.0, 4.0)
    row_scale = jnp.exp(jax.random.uniform(jax.random.fold_in(anchor, 2), (TOKENS, 1), jnp.float32, -0.5 * math.log(10.0), 0.5 * math.log(10.0)))
    column_scale = jnp.exp(jax.random.uniform(jax.random.fold_in(anchor, 3), (1, N), jnp.float32, -0.5 * math.log(10.0), 0.5 * math.log(10.0)))
    values = noise * row_scale * column_scale
    return values.astype(jnp.bfloat16)


def shard_levels(rng, extent, pieces, least, largest):
    loudness, own = 1.0, jax.random.fold_in(rng, 6)
    for axis_at, shards_of in pieces:
        heights = jnp.exp(jax.random.uniform(jax.random.fold_in(own, axis_at), (shards_of,), jnp.float32, least / len(pieces), largest / len(pieces)))
        loudness = loudness * jnp.repeat(heights, extent[axis_at] // shards_of).reshape([-1 if axis == axis_at else 1 for axis in range(len(extent))])
    return loudness


def normal_values(key, extent, scale, bound, pieces=(), held_as=jnp.bfloat16):
    values = scale * jax.random.normal(key, extent, jnp.float32)
    if pieces:
        values = values * shard_levels(key, extent, pieces, -0.22, 0.18)
    return jnp.clip(values, -bound, bound).astype(held_as)


def setup_inputs(seed: int = 0) -> dict:
    seeds = jax.random.split(jax.random.key(seed), 7)
    inputs = draw_inputs(jax.random.fold_in(seeds[6], 71), 0)
    gate_logits = normal_values(seeds[1], (TOKENS, N), 1.0, 5.0, ((0, 32),))
    step_sizes = draw_step_sizes(jax.random.fold_in(seeds[6], 71), 0)
    decay_rates = draw_decay_rates(jax.random.fold_in(seeds[6], 71), 0)
    skip_gain = jnp.clip(jax.random.uniform(seeds[4], (N,), jnp.float32, 0.3, 0.8), 0.3, 0.8)
    norm_gain = jnp.clip(1.0 + 0.15 * jax.random.normal(seeds[5], (N,), jnp.float32), 0.25, 1.75)
    return {"inputs": inputs, "gate_logits": gate_logits, "step_sizes": step_sizes, "decay_rates": decay_rates, "skip_gain": skip_gain, "norm_gain": norm_gain}


norm_epsilon = 1e-05

def combine_pairs(earlier, later):
    return (earlier[0] * later[0], later[0] * earlier[1] + later[1])

def reference(inputs, gate_logits, step_sizes, decay_rates, skip_gain, norm_gain):
    block_count = TOKENS // TOK_DEV
    input_blocks = inputs.reshape(block_count, TOK_DEV, N)
    gate_blocks = gate_logits.reshape(block_count, TOK_DEV, N)
    step_blocks = step_sizes.reshape(block_count, TOK_DEV, HEADS)

    def advance(carried, block):
        block_inputs, block_gate, block_steps = block
        widened = jnp.repeat(block_steps.astype(jnp.float32), HEAD_SIZE, axis=1) * decay_rates[None, :]
        decays = jnp.exp(-widened)
        values = block_inputs.astype(jnp.float32)
        drives = jnp.sqrt(-jnp.expm1(-2.0 * widened)) * values
        products, local_states = lax.associative_scan(combine_pairs, (decays, drives), axis=0)
        states = local_states + products * carried[None, :]
        mixed = (states + skip_gain[None, :] * values).astype(jnp.bfloat16)
        mixed = lax.optimization_barrier(mixed)
        gated = mixed.astype(jnp.float32) * jax.nn.silu(block_gate.astype(jnp.float32))
        factor = lax.rsqrt(lax.optimization_barrier(jnp.mean(gated * gated, axis=1, keepdims=True)) + norm_epsilon)
        result = (gated * factor * norm_gain[None, :]).astype(jnp.bfloat16)
        return (states[-1], result)
    start_state = jnp.zeros((N,), jnp.float32)
    final_state, results = lax.scan(advance, start_state, (input_blocks, gate_blocks, step_blocks))
    return results.reshape(TOKENS, N)
```

```python
import functools

import jax
import jax.numpy as jnp
from jax import lax
from jax.experimental import pallas as pl
from jax.experimental.pallas import tpu as pltpu
from jax.sharding import PartitionSpec as P

norm_epsilon = 1e-05
MESH = pl.DeviceIdType.MESH
LANES = 128
ROWS = 8
CHUNKS = 4
EARLY = 2


def order_table(tokens):
    run = tokens // ROWS
    row = lax.broadcasted_iota(jnp.int32, (tokens, tokens), 0)
    col = lax.broadcasted_iota(jnp.int32, (tokens, tokens), 1)
    return ((row % ROWS) * run + row // ROWS == col).astype(jnp.float32).astype(jnp.bfloat16)


def head_steps(steps, head, rate):
    heads = steps.shape[1]
    pick = lax.broadcasted_iota(jnp.int32, (heads, LANES), 0) == head
    table = pick.astype(jnp.float32).astype(jnp.bfloat16)
    return jnp.dot(steps, table, preferred_element_type=jnp.float32) * rate


def decay_and_scale(widened):
    decay = jnp.exp(-widened)
    twice = widened + widened
    series = twice * (1.0 + twice * (twice * (1.0 / 6.0) - 0.5))
    kept = jnp.where(twice < 0.0625, series, 1.0 - decay * decay)
    scale = kept * lax.rsqrt(jnp.maximum(kept, 1e-37))
    return decay, scale


def across_rows(prod, state):
    row = lax.broadcasted_iota(jnp.int32, prod.shape, 0)
    step = 1
    while step < ROWS:
        before_prod = jnp.where(row < step, 1.0, pltpu.roll(prod, step, 0))
        before_state = jnp.where(row < step, 0.0, pltpu.roll(state, step, 0))
        state = prod * before_state + state
        prod = prod * before_prod
        step *= 2
    return prod, state


def kernel(
    x_hbm, gate_hbm, steps_ref, rates_ref, skip_ref, gain_ref,
    out_ref,
    gated_all, x_loc, gate, recv, order, steps_in, steps_order, steps_mine,
    tot_prod, tot_state, block_out, block_in, carry_out, carry_in, sums, sums_plain,
    load_sem, x_send, x_recv, step_send, step_recv, block_send, block_recv, carry_send, carry_recv,
    *, tm_count, chan_count,
):
    me_tm = lax.axis_index("tm")
    me = lax.axis_index("chan")
    channels = x_loc.shape[1]
    heads = channels // LANES
    rows = gate.shape[0]
    run = rows // ROWS
    width = channels // CHUNKS
    chunk_heads = heads // CHUNKS

    load_x = pltpu.make_async_copy(x_hbm, x_loc, load_sem.at[0])
    load_own = pltpu.make_async_copy(x_hbm.at[pl.ds(me * rows, rows)], recv.at[me], load_sem.at[1])
    load_gate = pltpu.make_async_copy(gate_hbm, gate, load_sem.at[2])
    load_x.start()
    barrier = pltpu.get_barrier_semaphore()
    for d in range(1, chan_count):
        pl.semaphore_signal(
            barrier, 1, device_id={"chan": lax.rem(me + d, chan_count)}, device_id_type=MESH
        )

    def greet(k, _):
        pl.semaphore_signal(
            barrier, 1, device_id={"tm": lax.rem(me_tm + k, tm_count)}, device_id_type=MESH
        )
        return 0

    lax.fori_loop(1, tm_count, greet, 0)
    load_own.start()
    load_gate.start()

    order[...] = order_table(rows)
    def order_steps(steps):
        return lax.dot_general(
            order[...], steps, (((1,), (1,)), ((), ())), preferred_element_type=jnp.float32
        ).astype(jnp.bfloat16)

    for i in range(chan_count):
        steps_mine[i] = order_steps(steps_ref[:, i * rows:(i + 1) * rows])

    def x_copy(s, d):
        peer = lax.rem(me + d, chan_count)
        cols = pl.ds(pl.multiple_of(s * width, width), width)
        return pltpu.make_async_remote_copy(
            src_ref=x_loc.at[pl.ds(pl.multiple_of(peer * rows, rows), rows), cols],
            dst_ref=recv.at[me, :, cols],
            send_sem=x_send.at[s, d],
            recv_sem=x_recv.at[s, d],
            device_id={"chan": peer},
            device_id_type=MESH,
        )

    def step_copy(d):
        peer = lax.rem(me + d, chan_count)
        return pltpu.make_async_remote_copy(
            src_ref=steps_ref.at[:, pl.ds(pl.multiple_of(peer * rows, rows), rows)],
            dst_ref=steps_in.at[me],
            send_sem=step_send.at[d], recv_sem=step_recv.at[d],
            device_id={"chan": peer}, device_id_type=MESH,
        )

    def carry_copy(d):
        peer = lax.rem(me + d, chan_count)
        return pltpu.make_async_remote_copy(
            src_ref=carry_out.at[peer], dst_ref=carry_in.at[me],
            send_sem=carry_send.at[d], recv_sem=carry_recv.at[d],
            device_id={"chan": peer}, device_id_type=MESH,
        )

    def block_copy(k):
        return pltpu.make_async_remote_copy(
            src_ref=block_out, dst_ref=block_in.at[me_tm],
            send_sem=block_send.at[k], recv_sem=block_recv.at[k],
            device_id={"tm": lax.rem(me_tm + k, tm_count)}, device_id_type=MESH,
        )

    load_x.wait()
    pl.semaphore_wait(barrier, tm_count - 1 + chan_count - 1)
    for d in range(1, chan_count):
        x_copy(0, d).start()
    for d in range(1, chan_count):
        step_copy(d).start()
    for s in range(1, EARLY):
        for d in range(1, chan_count):
            x_copy(s, d).start()

    def total_head(head, _):
        cols = pl.ds(pl.multiple_of(head * LANES, LANES), LANES)
        rate = rates_ref[pl.ds(me * heads + head, 1), :]
        block_prod = jnp.ones((1, LANES), jnp.float32)
        block_state = jnp.zeros((1, LANES), jnp.float32)
        for i in range(chan_count):
            values = jnp.dot(
                order[...], x_loc[i * rows:(i + 1) * rows, cols],
                preferred_element_type=jnp.float32,
            )
            widened = head_steps(steps_mine[i], head, rate)
            prod = state = None
            for j in range(run):
                here = slice(j * ROWS, (j + 1) * ROWS)
                decay, scale = decay_and_scale(widened[here])
                drive = scale * values[here]
                prod = decay if j == 0 else prod * decay
                state = drive if j == 0 else decay * state + drive
            prod, state = across_rows(prod, state)
            last_prod, last_state = prod[ROWS - 1:], state[ROWS - 1:]
            tot_prod[i, :, cols] = last_prod
            tot_state[i, :, cols] = last_state
            block_state = last_prod * block_state + last_state
            block_prod = block_prod * last_prod
        block_out[0, :, cols] = block_prod
        block_out[1, :, cols] = block_state
        return 0

    lax.fori_loop(0, heads, total_head, 0)

    def send_block(k, _):
        block_copy(k).start()
        return 0

    lax.fori_loop(1, tm_count, send_block, 0)
    block_in[me_tm] = block_out[...]
    load_own.wait()
    load_gate.wait()
    sums[...] = jnp.zeros_like(sums)

    def take_block(k, _):
        block_copy(k).wait()
        return 0

    lax.fori_loop(1, tm_count, take_block, 0)

    def fold(k, carried):
        new = block_in[k, 0] * carried + block_in[k, 1]
        return jnp.where(k < me_tm, new, carried)

    carried = lax.fori_loop(0, tm_count, fold, jnp.zeros((1, channels), jnp.float32))
    for i in range(chan_count):
        carry_out[i] = carried
        carried = tot_prod[i] * carried + tot_state[i]
    carry_in[me] = carry_out[me]
    for d in range(1, chan_count):
        carry_copy(d).start()
    for s in range(EARLY, CHUNKS):
        for d in range(1, chan_count):
            x_copy(s, d).start()

    def state_head(source, head):
        cols = pl.ds(pl.multiple_of(head * LANES, LANES), LANES)
        whole = source * heads + head
        wide_cols = pl.ds(pl.multiple_of(whole * LANES, LANES), LANES)
        rate = rates_ref[pl.ds(whole, 1), :]
        skip = skip_ref[pl.ds(whole, 1), :]
        carried = carry_in[source, :, cols]
        values = jnp.dot(order[...], recv[source, :, cols], preferred_element_type=jnp.float32)
        logits = jnp.dot(order[...], gate[:, wide_cols], preferred_element_type=jnp.float32)
        widened = head_steps(steps_order[source], head, rate)
        prods, states = [], []
        for j in range(run):
            here = slice(j * ROWS, (j + 1) * ROWS)
            decay, scale = decay_and_scale(widened[here])
            drive = scale * values[here]
            prods.append(decay if j == 0 else prods[-1] * decay)
            states.append(drive if j == 0 else decay * states[-1] + drive)
        prod, state = across_rows(prods[-1], states[-1])
        ends = state + prod * carried
        row = lax.broadcasted_iota(jnp.int32, ends.shape, 0)
        entering = jnp.where(row < 1, carried, pltpu.roll(ends, 1, 0))
        for j in range(run):
            here = slice(j * ROWS, (j + 1) * ROWS)
            mixed = states[j] + prods[j] * entering + skip * values[here]
            mixed = mixed.astype(jnp.bfloat16).astype(jnp.float32)
            logit = logits[here]
            gated = mixed * (logit * (0.5 + 0.5 * jnp.tanh(0.5 * logit)))
            gated_all[whole, pl.ds(j, ROWS, stride=run), :] = gated
            sums[here, :] += gated * gated

    steps_order[me] = order_steps(steps_ref[:, pl.ds(pl.multiple_of(me * rows, rows), rows)])

    def own_head(head, _):
        state_head(me, head)
        return 0

    lax.fori_loop(0, heads, own_head, 0)
    for d in range(1, chan_count):
        step_copy(d).wait()
        carry_copy(d).wait()
        source = lax.rem(me + chan_count - d, chan_count)
        steps_order[source] = order_steps(steps_in[source])

    def arrive(t, _):
        s = t // (chan_count - 1)
        d = t % (chan_count - 1) + 1
        x_copy(s, d).wait_recv()
        source = lax.rem(me + chan_count - d, chan_count)

        def one(h, _):
            state_head(source, s * chunk_heads + h)
            return 0

        lax.fori_loop(0, chunk_heads, one, 0)
        return 0

    lax.fori_loop(0, CHUNKS * (chan_count - 1), arrive, 0)

    for j in range(run):
        sums_plain[pl.ds(j, ROWS, stride=run), :] = sums[j * ROWS:(j + 1) * ROWS, :]
    mean = jnp.sum(sums_plain[...], axis=1, keepdims=True) * (1.0 / gate.shape[1])
    factor = jnp.broadcast_to(lax.rsqrt(mean + norm_epsilon), sums_plain.shape)

    def finish(head, _):
        cols = pl.ds(pl.multiple_of(head * LANES, LANES), LANES)
        gain = gain_ref[pl.ds(head, 1), :]
        out_ref[:, cols] = (gated_all[head] * factor * gain).astype(out_ref.dtype)
        return 0

    lax.fori_loop(0, gate.shape[1] // LANES, finish, 0)

    def sent(t, _):
        x_copy(t // (chan_count - 1), t % (chan_count - 1) + 1).wait_send()
        return 0

    lax.fori_loop(0, CHUNKS * (chan_count - 1), sent, 0)


def per_device(tm_count, chan_count, inputs, gate_logits, step_sizes, decay_rates, skip_gain, norm_gain):
    tokens, channels = inputs.shape
    rows, width = gate_logits.shape
    heads = channels // LANES
    f32, bf16 = jnp.float32, jnp.bfloat16
    vmem = pl.BlockSpec(memory_space=pltpu.VMEM)
    hbm = pl.BlockSpec(memory_space=pl.ANY)
    dma = pltpu.SemaphoreType.DMA
    return pl.pallas_call(
        functools.partial(kernel, tm_count=tm_count, chan_count=chan_count),
        out_shape=jax.ShapeDtypeStruct((rows, width), bf16),
        in_specs=[hbm, hbm, vmem, vmem, vmem, vmem],
        out_specs=vmem,
        scratch_shapes=[
            pltpu.VMEM((width // LANES, rows, LANES), f32),
            pltpu.VMEM((tokens, channels), bf16),
            pltpu.VMEM((rows, width), bf16),
            pltpu.VMEM((chan_count, rows, channels), bf16),
            pltpu.VMEM((rows, rows), bf16),
            pltpu.VMEM((chan_count, heads, rows), bf16),
            pltpu.VMEM((chan_count, rows, heads), bf16),
            pltpu.VMEM((chan_count, rows, heads), bf16),
            pltpu.VMEM((chan_count, 1, channels), f32),
            pltpu.VMEM((chan_count, 1, channels), f32),
            pltpu.VMEM((2, 1, channels), f32),
            pltpu.VMEM((tm_count, 2, 1, channels), f32),
            pltpu.VMEM((chan_count, 1, channels), f32),
            pltpu.VMEM((chan_count, 1, channels), f32),
            pltpu.VMEM((rows, LANES), f32),
            pltpu.VMEM((rows, LANES), f32),
            dma((3,)),
            dma((CHUNKS, chan_count)),
            dma((CHUNKS, chan_count)),
            dma((chan_count,)),
            dma((chan_count,)),
            dma((tm_count,)),
            dma((tm_count,)),
            dma((chan_count,)),
            dma((chan_count,)),
        ],
        compiler_params=pltpu.CompilerParams(
            collective_id=0, has_side_effects=True, vmem_limit_bytes=56 * 1024 * 1024
        ),
    )(
        inputs, gate_logits, step_sizes.T,
        decay_rates.reshape(-1, LANES), skip_gain.reshape(-1, LANES), norm_gain.reshape(-1, LANES),
    )


def solution(mesh):
    in_specs = (P("tm", "chan"), P(("tm", "chan"), None), P("tm", "chan"), P(), P(), P())
    out_specs = P(("tm", "chan"), None)
    body = functools.partial(per_device, mesh.shape["tm"], mesh.shape["chan"])
    return jax.shard_map(
        body, mesh=mesh, in_specs=in_specs, out_specs=out_specs, check_vma=False
    )
```

```python
import functools

import jax
import jax.numpy as jnp
from jax import lax
from jax.experimental import pallas as pl
from jax.experimental.pallas import tpu as pltpu
from jax.sharding import PartitionSpec as P

norm_epsilon = 1e-05
MESH = pl.DeviceIdType.MESH
LANES = 128
ROWS = 8
CHUNKS = 4
EARLY = 2
FINISH = 8


def order_table(tokens):
    run = tokens // ROWS
    row = lax.broadcasted_iota(jnp.int32, (tokens, tokens), 0)
    col = lax.broadcasted_iota(jnp.int32, (tokens, tokens), 1)
    return ((row % ROWS) * run + row // ROWS == col).astype(jnp.float32).astype(jnp.bfloat16)


def head_steps(steps, head, rate):
    heads = steps.shape[1]
    pick = lax.broadcasted_iota(jnp.int32, (heads, LANES), 0) == head
    table = pick.astype(jnp.float32).astype(jnp.bfloat16)
    return jnp.dot(steps, table, preferred_element_type=jnp.float32) * rate


def decay_and_scale(widened):
    decay = jnp.exp(-widened)
    twice = widened + widened
    series = twice * (1.0 + twice * (twice * (1.0 / 6.0) - 0.5))
    kept = jnp.where(twice < 0.0625, series, 1.0 - decay * decay)
    scale = kept * lax.rsqrt(jnp.maximum(kept, 1e-37))
    return decay, scale


def across_rows(prod, state):
    row = lax.broadcasted_iota(jnp.int32, prod.shape, 0)
    step = 1
    while step < ROWS:
        before_prod = jnp.where(row < step, 1.0, pltpu.roll(prod, step, 0))
        before_state = jnp.where(row < step, 0.0, pltpu.roll(state, step, 0))
        state = prod * before_state + state
        prod = prod * before_prod
        step *= 2
    return prod, state


def kernel(
    x_hbm, gate_hbm, steps_ref, rates_ref, skip_ref, gain_ref,
    gated_all, factor_ref,
    x_loc, gate, recv, order, steps_in, steps_order, steps_mine,
    tot_prod, tot_state, block_out, block_in, carry_out, carry_in, sums, sums_plain,
    decays, scales, prods, silus,
    load_sem, x_send, x_recv, step_send, step_recv, block_send, block_recv, carry_send, carry_recv,
    *, tm_count, chan_count,
):
    me_tm = lax.axis_index("tm")
    me = lax.axis_index("chan")
    channels = x_loc.shape[1]
    heads = channels // LANES
    rows = gate.shape[0]
    run = rows // ROWS
    width = channels // CHUNKS
    chunk_heads = heads // CHUNKS

    load_x = pltpu.make_async_copy(x_hbm, x_loc, load_sem.at[0])
    load_own = pltpu.make_async_copy(x_hbm.at[pl.ds(me * rows, rows)], recv.at[me], load_sem.at[1])
    load_gate = pltpu.make_async_copy(gate_hbm, gate, load_sem.at[2])
    load_x.start()
    barrier = pltpu.get_barrier_semaphore()
    for d in range(1, chan_count):
        pl.semaphore_signal(
            barrier, 1, device_id={"chan": lax.rem(me + d, chan_count)}, device_id_type=MESH
        )

    def greet(k, _):
        pl.semaphore_signal(
            barrier, 1, device_id={"tm": lax.rem(me_tm + k, tm_count)}, device_id_type=MESH
        )
        return 0

    lax.fori_loop(1, tm_count, greet, 0)
    load_own.start()
    load_gate.start()

    order[...] = order_table(rows)
    def order_steps(steps):
        return lax.dot_general(
            order[...], steps, (((1,), (1,)), ((), ())), preferred_element_type=jnp.float32
        ).astype(jnp.bfloat16)

    for i in range(chan_count):
        steps_mine[i] = order_steps(steps_ref[:, i * rows:(i + 1) * rows])

    def x_copy(s, d):
        peer = lax.rem(me + d, chan_count)
        cols = pl.ds(pl.multiple_of(s * width, width), width)
        return pltpu.make_async_remote_copy(
            src_ref=x_loc.at[pl.ds(pl.multiple_of(peer * rows, rows), rows), cols],
            dst_ref=recv.at[me, :, cols],
            send_sem=x_send.at[s, d],
            recv_sem=x_recv.at[s, d],
            device_id={"chan": peer},
            device_id_type=MESH,
        )

    def step_copy(d):
        peer = lax.rem(me + d, chan_count)
        return pltpu.make_async_remote_copy(
            src_ref=steps_ref.at[:, pl.ds(pl.multiple_of(peer * rows, rows), rows)],
            dst_ref=steps_in.at[me],
            send_sem=step_send.at[d], recv_sem=step_recv.at[d],
            device_id={"chan": peer}, device_id_type=MESH,
        )

    def carry_copy(d):
        peer = lax.rem(me + d, chan_count)
        return pltpu.make_async_remote_copy(
            src_ref=carry_out.at[peer], dst_ref=carry_in.at[me],
            send_sem=carry_send.at[d], recv_sem=carry_recv.at[d],
            device_id={"chan": peer}, device_id_type=MESH,
        )

    def block_copy(k):
        return pltpu.make_async_remote_copy(
            src_ref=block_out, dst_ref=block_in.at[me_tm],
            send_sem=block_send.at[k], recv_sem=block_recv.at[k],
            device_id={"tm": lax.rem(me_tm + k, tm_count)}, device_id_type=MESH,
        )

    load_x.wait()
    pl.semaphore_wait(barrier, tm_count - 1 + chan_count - 1)
    for d in range(1, chan_count):
        x_copy(0, d).start()
    for d in range(1, chan_count):
        step_copy(d).start()
    for s in range(1, EARLY):
        for d in range(1, chan_count):
            x_copy(s, d).start()

    def total_head(head, _):
        cols = pl.ds(pl.multiple_of(head * LANES, LANES), LANES)
        rate = rates_ref[pl.ds(me * heads + head, 1), :]
        block_prod = jnp.ones((1, LANES), jnp.float32)
        block_state = jnp.zeros((1, LANES), jnp.float32)
        for i in range(chan_count):
            values = jnp.dot(
                order[...], x_loc[i * rows:(i + 1) * rows, cols],
                preferred_element_type=jnp.float32,
            )
            widened = head_steps(steps_mine[i], head, rate)
            prod = state = None
            for j in range(run):
                here = slice(j * ROWS, (j + 1) * ROWS)
                decay, scale = decay_and_scale(widened[here])
                drive = scale * values[here]
                prod = decay if j == 0 else prod * decay
                state = drive if j == 0 else decay * state + drive
            prod, state = across_rows(prod, state)
            last_prod, last_state = prod[ROWS - 1:], state[ROWS - 1:]
            tot_prod[i, :, cols] = last_prod
            tot_state[i, :, cols] = last_state
            block_state = last_prod * block_state + last_state
            block_prod = block_prod * last_prod
        block_out[0, :, cols] = block_prod
        block_out[1, :, cols] = block_state
        return 0

    lax.fori_loop(0, heads, total_head, 0)

    def send_block(k, _):
        block_copy(k).start()
        return 0

    lax.fori_loop(1, tm_count, send_block, 0)
    block_in[me_tm] = block_out[...]
    load_own.wait()
    load_gate.wait()
    sums[...] = jnp.zeros_like(sums)

    def take_block(k, _):
        block_copy(k).wait()
        return 0

    lax.fori_loop(1, tm_count, take_block, 0)

    def fold(k, carried):
        new = block_in[k, 0] * carried + block_in[k, 1]
        return jnp.where(k < me_tm, new, carried)

    carried = lax.fori_loop(0, tm_count, fold, jnp.zeros((1, channels), jnp.float32))
    for i in range(chan_count):
        carry_out[i] = carried
        carried = tot_prod[i] * carried + tot_state[i]
    carry_in[me] = carry_out[me]
    for d in range(1, chan_count):
        carry_copy(d).start()
    for s in range(EARLY, CHUNKS):
        for d in range(1, chan_count):
            x_copy(s, d).start()

    def places(source, head):
        whole = source * heads + head
        return (
            whole,
            pl.ds(pl.multiple_of(head * LANES, LANES), LANES),
            pl.ds(pl.multiple_of(whole * LANES, LANES), LANES),
        )

    def prepare_head(source, head):
        whole, _, wide_cols = places(source, head)
        rate = rates_ref[pl.ds(whole, 1), :]
        logits = jnp.dot(order[...], gate[:, wide_cols], preferred_element_type=jnp.float32)
        widened = head_steps(steps_order[source], head, rate)
        prod = None
        for j in range(run):
            here = slice(j * ROWS, (j + 1) * ROWS)
            decay, scale = decay_and_scale(widened[here])
            prod = decay if j == 0 else prod * decay
            logit = logits[here]
            decays[whole, here, :] = decay
            scales[whole, here, :] = scale
            prods[whole, here, :] = prod
            silus[whole, here, :] = logit * (0.5 + 0.5 * jnp.tanh(0.5 * logit))

    def state_head(source, head):
        whole, cols, _ = places(source, head)
        skip = skip_ref[pl.ds(whole, 1), :]
        gain = gain_ref[pl.ds(whole, 1), :]
        carried = carry_in[source, :, cols]
        values = jnp.dot(order[...], recv[source, :, cols], preferred_element_type=jnp.float32)
        states = []
        for j in range(run):
            here = slice(j * ROWS, (j + 1) * ROWS)
            drive = scales[whole, here, :] * values[here]
            states.append(drive if j == 0 else decays[whole, here, :] * states[-1] + drive)
        prod, state = across_rows(prods[whole, (run - 1) * ROWS:, :], states[-1])
        ends = state + prod * carried
        row = lax.broadcasted_iota(jnp.int32, ends.shape, 0)
        entering = jnp.where(row < 1, carried, pltpu.roll(ends, 1, 0))
        for j in range(run):
            here = slice(j * ROWS, (j + 1) * ROWS)
            mixed = states[j] + prods[whole, here, :] * entering + skip * values[here]
            gated = mixed.astype(jnp.bfloat16).astype(jnp.float32) * silus[whole, here, :]
            gated_all[whole, pl.ds(j, ROWS, stride=run), :] = gated * gain
            sums[here, :] += gated * gated

    steps_order[me] = order_steps(steps_ref[:, pl.ds(pl.multiple_of(me * rows, rows), rows)])

    for d in range(1, chan_count):
        step_copy(d).wait()
        source = lax.rem(me + chan_count - d, chan_count)
        steps_order[source] = order_steps(steps_in[source])

    def prepare(t, _):
        prepare_head(t // heads, t % heads)
        return 0

    lax.fori_loop(0, chan_count * heads, prepare, 0)

    def own_head(head, _):
        state_head(me, head)
        return 0

    lax.fori_loop(0, heads, own_head, 0)
    for d in range(1, chan_count):
        carry_copy(d).wait()

    def arrive(t, _):
        s = t // (chan_count - 1)
        d = t % (chan_count - 1) + 1
        x_copy(s, d).wait_recv()
        source = lax.rem(me + chan_count - d, chan_count)

        def one(h, _):
            state_head(source, s * chunk_heads + h)
            return 0

        lax.fori_loop(0, chunk_heads, one, 0)
        return 0

    lax.fori_loop(0, CHUNKS * (chan_count - 1), arrive, 0)

    for j in range(run):
        sums_plain[pl.ds(j, ROWS, stride=run), :] = sums[j * ROWS:(j + 1) * ROWS, :]
    mean = jnp.sum(sums_plain[...], axis=1, keepdims=True) * (1.0 / gate.shape[1])
    factor_ref[...] = jnp.broadcast_to(lax.rsqrt(mean + norm_epsilon), factor_ref.shape)

    def sent(t, _):
        x_copy(t // (chan_count - 1), t % (chan_count - 1) + 1).wait_send()
        return 0

    lax.fori_loop(0, CHUNKS * (chan_count - 1), sent, 0)


def scale_kernel(gated_ref, factor_ref, out_hbm, staged, sems):
    heads, rows, _ = gated_ref.shape
    part = heads // FINISH
    copies = []
    for piece in range(FINISH):
        for inner in range(part):
            head = piece * part + inner
            value = gated_ref[head] * factor_ref[...]
            staged[:, head * LANES:(head + 1) * LANES] = value.astype(staged.dtype)
        cols = pl.ds(piece * part * LANES, part * LANES)
        copy = pltpu.make_async_copy(staged.at[:, cols], out_hbm.at[:, cols], sems.at[piece])
        copy.start()
        copies.append(copy)
    for copy in copies:
        copy.wait()


def per_device(tm_count, chan_count, inputs, gate_logits, step_sizes, decay_rates, skip_gain, norm_gain):
    tokens, channels = inputs.shape
    rows, width = gate_logits.shape
    heads = channels // LANES
    f32, bf16 = jnp.float32, jnp.bfloat16
    vmem = pl.BlockSpec(memory_space=pltpu.VMEM)
    hbm = pl.BlockSpec(memory_space=pltpu.HBM)
    dma = pltpu.SemaphoreType.DMA
    gated, factor = pl.pallas_call(
        functools.partial(kernel, tm_count=tm_count, chan_count=chan_count),
        out_shape=(
            pltpu.VMEM((width // LANES, rows, LANES), f32),
            pltpu.VMEM((rows, LANES), f32),
        ),
        in_specs=[hbm, hbm, vmem, vmem, vmem, vmem],
        out_specs=(vmem, vmem),
        scratch_shapes=[
            pltpu.VMEM((tokens, channels), bf16),
            pltpu.VMEM((rows, width), bf16),
            pltpu.VMEM((chan_count, rows, channels), bf16),
            pltpu.VMEM((rows, rows), bf16),
            pltpu.VMEM((chan_count, heads, rows), bf16),
            pltpu.VMEM((chan_count, rows, heads), bf16),
            pltpu.VMEM((chan_count, rows, heads), bf16),
            pltpu.VMEM((chan_count, 1, channels), f32),
            pltpu.VMEM((chan_count, 1, channels), f32),
            pltpu.VMEM((2, 1, channels), f32),
            pltpu.VMEM((tm_count, 2, 1, channels), f32),
            pltpu.VMEM((chan_count, 1, channels), f32),
            pltpu.VMEM((chan_count, 1, channels), f32),
            pltpu.VMEM((rows, LANES), f32),
            pltpu.VMEM((rows, LANES), f32),
            *[pltpu.VMEM((width // LANES, rows, LANES), f32)] * 4,
            dma((3,)),
            dma((CHUNKS, chan_count)),
            dma((CHUNKS, chan_count)),
            dma((chan_count,)),
            dma((chan_count,)),
            dma((tm_count,)),
            dma((tm_count,)),
            dma((chan_count,)),
            dma((chan_count,)),
        ],
        compiler_params=pltpu.CompilerParams(
            collective_id=0, has_side_effects=True, vmem_limit_bytes=58 * 1024 * 1024
        ),
    )(
        inputs, gate_logits, step_sizes.T,
        decay_rates.reshape(-1, LANES), skip_gain.reshape(-1, LANES), norm_gain.reshape(-1, LANES),
    )
    return pl.pallas_call(
        scale_kernel,
        out_shape=jax.ShapeDtypeStruct((rows, width), bf16),
        in_specs=[vmem, vmem],
        out_specs=hbm,
        scratch_shapes=[pltpu.VMEM((rows, width), bf16), dma((FINISH,))],
        compiler_params=pltpu.CompilerParams(vmem_limit_bytes=16 * 1024 * 1024),
    )(
        pltpu.with_memory_space_constraint(gated, pltpu.VMEM),
        pltpu.with_memory_space_constraint(factor, pltpu.VMEM),
    )


def solution(mesh):
    in_specs = (P("tm", "chan"), P(("tm", "chan"), None), P("tm", "chan"), P(), P(), P())
    out_specs = P(("tm", "chan"), None)
    body = functools.partial(per_device, mesh.shape["tm"], mesh.shape["chan"])
    return jax.shard_map(
        body, mesh=mesh, in_specs=in_specs, out_specs=out_specs, check_vma=False
    )
```

```python
import functools

import jax
import jax.numpy as jnp
from jax import lax
from jax.experimental import pallas as pl
from jax.experimental.pallas import tpu as pltpu
from jax.sharding import PartitionSpec as P

norm_epsilon = 1e-05
MESH = pl.DeviceIdType.MESH
LANES = 128
ROWS = 8
CHUNKS = 4
EARLY = 2
FINISH = 8


def order_table(tokens):
    run = tokens // ROWS
    row = lax.broadcasted_iota(jnp.int32, (tokens, tokens), 0)
    col = lax.broadcasted_iota(jnp.int32, (tokens, tokens), 1)
    return ((row % ROWS) * run + row // ROWS == col).astype(jnp.float32).astype(jnp.bfloat16)


def head_steps(steps, head, rate):
    heads = steps.shape[1]
    pick = lax.broadcasted_iota(jnp.int32, (heads, LANES), 0) == head
    table = pick.astype(jnp.float32).astype(jnp.bfloat16)
    return jnp.dot(steps, table, preferred_element_type=jnp.float32) * rate


def decay_and_scale(widened):
    decay = jnp.exp(-widened)
    twice = widened + widened
    series = twice * (1.0 + twice * (twice * (1.0 / 6.0) - 0.5))
    kept = jnp.where(twice < 0.0625, series, 1.0 - decay * decay)
    scale = kept * lax.rsqrt(jnp.maximum(kept, 1e-37))
    return decay, scale


def upper(index, r):
    return lax.rem(index // (1 << r), 2)


def partner(index, r):
    return index + (1 << r) * (1 - 2 * upper(index, r))


def across_rows(prod, state):
    row = lax.broadcasted_iota(jnp.int32, prod.shape, 0)
    step = 1
    while step < ROWS:
        before_prod = jnp.where(row < step, 1.0, pltpu.roll(prod, step, 0))
        before_state = jnp.where(row < step, 0.0, pltpu.roll(state, step, 0))
        state = prod * before_state + state
        prod = prod * before_prod
        step *= 2
    return prod, state


def kernel(
    x_hbm, gate_hbm, steps_ref, rates_ref, skip_ref, gain_ref,
    gated_all, factor_ref,
    x_loc, gate, recv, order, steps_in, steps_order, steps_mine,
    tot_prod, tot_state, block_out, block_in, carry_out, carry_in, sums, sums_plain,
    decays, scales, prods, silus,
    load_sem, x_send, x_recv, step_send, step_recv, block_send, block_recv, carry_send, carry_recv,
    from_left, from_right,
    *, tm_count, chan_count,
):
    me_tm = lax.axis_index("tm")
    me = lax.axis_index("chan")
    channels = x_loc.shape[1]
    heads = channels // LANES
    rows = gate.shape[0]
    run = rows // ROWS
    width = channels // CHUNKS
    chunk_heads = heads // CHUNKS

    load_x = pltpu.make_async_copy(x_hbm, x_loc, load_sem.at[0])
    load_own = pltpu.make_async_copy(x_hbm.at[pl.ds(me * rows, rows)], recv.at[me], load_sem.at[1])
    load_gate = pltpu.make_async_copy(gate_hbm, gate, load_sem.at[2])
    load_x.start()
    barrier = pltpu.get_barrier_semaphore()
    rounds = (tm_count - 1).bit_length()
    has_left, has_right = me >= 1, me + 1 < chan_count

    def greet(peer):
        pl.semaphore_signal(barrier, 1, device_id={"chan": peer}, device_id_type=MESH)

    pl.when(has_left)(lambda: greet(me - 1))
    pl.when(has_right)(lambda: greet(me + 1))
    for r in range(rounds):
        pl.semaphore_signal(barrier, 1, device_id={"tm": partner(me_tm, r)}, device_id_type=MESH)
    load_own.start()
    load_gate.start()

    order[...] = order_table(rows)
    def order_steps(steps):
        return lax.dot_general(
            order[...], steps, (((1,), (1,)), ((), ())), preferred_element_type=jnp.float32
        ).astype(jnp.bfloat16)

    for i in range(chan_count):
        steps_mine[i] = order_steps(steps_ref[:, i * rows:(i + 1) * rows])

    def x_copy(s, d):
        peer = lax.rem(me + d, chan_count)
        cols = pl.ds(pl.multiple_of(s * width, width), width)
        return pltpu.make_async_remote_copy(
            src_ref=x_loc.at[pl.ds(pl.multiple_of(peer * rows, rows), rows), cols],
            dst_ref=recv.at[me, :, cols],
            send_sem=x_send.at[s, d],
            recv_sem=x_recv.at[s, d],
            device_id={"chan": peer},
            device_id_type=MESH,
        )

    def step_copy(d):
        peer = lax.rem(me + d, chan_count)
        return pltpu.make_async_remote_copy(
            src_ref=steps_ref.at[:, pl.ds(pl.multiple_of(peer * rows, rows), rows)],
            dst_ref=steps_in.at[me],
            send_sem=step_send.at[d], recv_sem=step_recv.at[d],
            device_id={"chan": peer}, device_id_type=MESH,
        )

    def carry_copy(d):
        peer = lax.rem(me + d, chan_count)
        return pltpu.make_async_remote_copy(
            src_ref=carry_out.at[peer], dst_ref=carry_in.at[me],
            send_sem=carry_send.at[d], recv_sem=carry_recv.at[d],
            device_id={"chan": peer}, device_id_type=MESH,
        )

    def block_copy(r):
        return pltpu.make_async_remote_copy(
            src_ref=block_out.at[r], dst_ref=block_in.at[r],
            send_sem=block_send.at[r], recv_sem=block_recv.at[r],
            device_id={"tm": partner(me_tm, r)}, device_id_type=MESH,
        )

    load_x.wait()
    pl.semaphore_wait(barrier, rounds + has_left.astype(jnp.int32) + has_right.astype(jnp.int32))

    def begin(d):
        x_copy(0, d).start()
        step_copy(d).start()

    def tell(sem, peer):
        pl.semaphore_signal(sem, 1, device_id={"chan": peer}, device_id_type=MESH)

    for far in range(1, chan_count):
        right_is, left_is = me + far < chan_count, me >= far
        if far > 1:
            pl.when(has_right & (me + 1 >= far))(functools.partial(tell, from_left.at[far], me + 1))
            pl.when(has_left & (me - 1 + far < chan_count))(
                functools.partial(tell, from_right.at[far], me - 1)
            )
            pl.when(left_is)(lambda: pl.semaphore_wait(from_left.at[far], 1))
            pl.when(right_is)(lambda: pl.semaphore_wait(from_right.at[far], 1))
        pl.when(right_is)(functools.partial(begin, far))
        pl.when(left_is)(functools.partial(begin, chan_count - far))
    for s in range(1, EARLY):
        for d in range(1, chan_count):
            x_copy(s, d).start()

    def total_head(head, _):
        cols = pl.ds(pl.multiple_of(head * LANES, LANES), LANES)
        rate = rates_ref[pl.ds(me * heads + head, 1), :]
        block_prod = jnp.ones((1, LANES), jnp.float32)
        block_state = jnp.zeros((1, LANES), jnp.float32)
        for i in range(chan_count):
            values = jnp.dot(
                order[...], x_loc[i * rows:(i + 1) * rows, cols],
                preferred_element_type=jnp.float32,
            )
            widened = head_steps(steps_mine[i], head, rate)
            prod = state = None
            for j in range(run):
                here = slice(j * ROWS, (j + 1) * ROWS)
                decay, scale = decay_and_scale(widened[here])
                drive = scale * values[here]
                prod = decay if j == 0 else prod * decay
                state = drive if j == 0 else decay * state + drive
            prod, state = across_rows(prod, state)
            last_prod, last_state = prod[ROWS - 1:], state[ROWS - 1:]
            tot_prod[i, :, cols] = last_prod
            tot_state[i, :, cols] = last_state
            block_state = last_prod * block_state + last_state
            block_prod = block_prod * last_prod
        block_out[0, 0, :, cols] = block_prod
        block_out[0, 1, :, cols] = block_state
        return 0

    lax.fori_loop(0, heads, total_head, 0)

    before_prod = jnp.ones((1, channels), jnp.float32)
    carried = jnp.zeros((1, channels), jnp.float32)
    for r in range(rounds):
        block_copy(r).start()
        if r == 0:
            load_own.wait()
            load_gate.wait()
            sums[...] = jnp.zeros_like(sums)
        block_copy(r).wait()
        their_prod, their_state = block_in[r, 0], block_in[r, 1]
        our_prod, our_state = block_out[r, 0], block_out[r, 1]
        late = upper(me_tm, r) == 1
        carried = jnp.where(late, before_prod * their_state + carried, carried)
        before_prod = jnp.where(late, before_prod * their_prod, before_prod)
        if r + 1 < rounds:
            block_out[r + 1, 0] = our_prod * their_prod
            block_out[r + 1, 1] = jnp.where(
                late, our_prod * their_state + our_state, their_prod * our_state + their_state
            )
    for i in range(chan_count):
        carry_out[i] = carried
        carried = tot_prod[i] * carried + tot_state[i]
    carry_in[me] = carry_out[me]
    for d in range(1, chan_count):
        carry_copy(d).start()
    for s in range(EARLY, CHUNKS):
        for d in range(1, chan_count):
            x_copy(s, d).start()

    def places(source, head):
        whole = source * heads + head
        return (
            whole,
            pl.ds(pl.multiple_of(head * LANES, LANES), LANES),
            pl.ds(pl.multiple_of(whole * LANES, LANES), LANES),
        )

    def prepare_head(source, head):
        whole, _, wide_cols = places(source, head)
        rate = rates_ref[pl.ds(whole, 1), :]
        logits = jnp.dot(order[...], gate[:, wide_cols], preferred_element_type=jnp.float32)
        widened = head_steps(steps_order[source], head, rate)
        prod = None
        for j in range(run):
            here = slice(j * ROWS, (j + 1) * ROWS)
            decay, scale = decay_and_scale(widened[here])
            prod = decay if j == 0 else prod * decay
            logit = logits[here]
            decays[whole, here, :] = decay
            scales[whole, here, :] = scale
            prods[whole, here, :] = prod
            silus[whole, here, :] = logit * (0.5 + 0.5 * jnp.tanh(0.5 * logit))

    def state_head(source, head):
        whole, cols, _ = places(source, head)
        skip = skip_ref[pl.ds(whole, 1), :]
        gain = gain_ref[pl.ds(whole, 1), :]
        carried = carry_in[source, :, cols]
        values = jnp.dot(order[...], recv[source, :, cols], preferred_element_type=jnp.float32)
        states = []
        for j in range(run):
            here = slice(j * ROWS, (j + 1) * ROWS)
            drive = scales[whole, here, :] * values[here]
            states.append(drive if j == 0 else decays[whole, here, :] * states[-1] + drive)
        prod, state = across_rows(prods[whole, (run - 1) * ROWS:, :], states[-1])
        ends = state + prod * carried
        row = lax.broadcasted_iota(jnp.int32, ends.shape, 0)
        entering = jnp.where(row < 1, carried, pltpu.roll(ends, 1, 0))
        for j in range(run):
            here = slice(j * ROWS, (j + 1) * ROWS)
            mixed = states[j] + prods[whole, here, :] * entering + skip * values[here]
            gated = mixed.astype(jnp.bfloat16).astype(jnp.float32) * silus[whole, here, :]
            gated_all[whole, pl.ds(j, ROWS, stride=run), :] = gated * gain
            sums[here, :] += gated * gated

    steps_order[me] = order_steps(steps_ref[:, pl.ds(pl.multiple_of(me * rows, rows), rows)])

    for d in range(1, chan_count):
        step_copy(d).wait()
        source = lax.rem(me + chan_count - d, chan_count)
        steps_order[source] = order_steps(steps_in[source])

    def prepare(t, _):
        prepare_head(t // heads, t % heads)
        return 0

    lax.fori_loop(0, chan_count * heads, prepare, 0)

    def own_head(head, _):
        state_head(me, head)
        return 0

    lax.fori_loop(0, heads, own_head, 0)
    for d in range(1, chan_count):
        carry_copy(d).wait()

    def arrive(t, _):
        s = t // (chan_count - 1)
        d = t % (chan_count - 1) + 1
        x_copy(s, d).wait_recv()
        source = lax.rem(me + chan_count - d, chan_count)

        def one(h, _):
            state_head(source, s * chunk_heads + h)
            return 0

        lax.fori_loop(0, chunk_heads, one, 0)
        return 0

    lax.fori_loop(0, CHUNKS * (chan_count - 1), arrive, 0)

    for j in range(run):
        sums_plain[pl.ds(j, ROWS, stride=run), :] = sums[j * ROWS:(j + 1) * ROWS, :]
    mean = jnp.sum(sums_plain[...], axis=1, keepdims=True) * (1.0 / gate.shape[1])
    factor_ref[...] = jnp.broadcast_to(lax.rsqrt(mean + norm_epsilon), factor_ref.shape)

    def sent(t, _):
        x_copy(t // (chan_count - 1), t % (chan_count - 1) + 1).wait_send()
        return 0

    lax.fori_loop(0, CHUNKS * (chan_count - 1), sent, 0)


def scale_kernel(gated_ref, factor_ref, out_hbm, staged, sems):
    heads, rows, _ = gated_ref.shape
    part = heads // FINISH
    copies = []
    for piece in range(FINISH):
        for inner in range(part):
            head = piece * part + inner
            value = gated_ref[head] * factor_ref[...]
            staged[:, head * LANES:(head + 1) * LANES] = value.astype(staged.dtype)
        cols = pl.ds(piece * part * LANES, part * LANES)
        copy = pltpu.make_async_copy(staged.at[:, cols], out_hbm.at[:, cols], sems.at[piece])
        copy.start()
        copies.append(copy)
    for copy in copies:
        copy.wait()


def per_device(tm_count, chan_count, inputs, gate_logits, step_sizes, decay_rates, skip_gain, norm_gain):
    tokens, channels = inputs.shape
    rows, width = gate_logits.shape
    heads = channels // LANES
    rounds = (tm_count - 1).bit_length()
    assert tm_count == 1 << rounds
    f32, bf16 = jnp.float32, jnp.bfloat16
    vmem = pl.BlockSpec(memory_space=pltpu.VMEM)
    hbm = pl.BlockSpec(memory_space=pltpu.HBM)
    dma = pltpu.SemaphoreType.DMA
    gated, factor = pl.pallas_call(
        functools.partial(kernel, tm_count=tm_count, chan_count=chan_count),
        out_shape=(
            pltpu.VMEM((width // LANES, rows, LANES), f32),
            pltpu.VMEM((rows, LANES), f32),
        ),
        in_specs=[hbm, hbm, vmem, vmem, vmem, vmem],
        out_specs=(vmem, vmem),
        scratch_shapes=[
            pltpu.VMEM((tokens, channels), bf16),
            pltpu.VMEM((rows, width), bf16),
            pltpu.VMEM((chan_count, rows, channels), bf16),
            pltpu.VMEM((rows, rows), bf16),
            pltpu.VMEM((chan_count, heads, rows), bf16),
            pltpu.VMEM((chan_count, rows, heads), bf16),
            pltpu.VMEM((chan_count, rows, heads), bf16),
            pltpu.VMEM((chan_count, 1, channels), f32),
            pltpu.VMEM((chan_count, 1, channels), f32),
            pltpu.VMEM((rounds, 2, 1, channels), f32),
            pltpu.VMEM((rounds, 2, 1, channels), f32),
            pltpu.VMEM((chan_count, 1, channels), f32),
            pltpu.VMEM((chan_count, 1, channels), f32),
            pltpu.VMEM((rows, LANES), f32),
            pltpu.VMEM((rows, LANES), f32),
            *[pltpu.VMEM((width // LANES, rows, LANES), f32)] * 4,
            dma((3,)),
            dma((CHUNKS, chan_count)),
            dma((CHUNKS, chan_count)),
            dma((chan_count,)),
            dma((chan_count,)),
            dma((rounds,)),
            dma((rounds,)),
            dma((chan_count,)),
            dma((chan_count,)),
            pltpu.SemaphoreType.REGULAR((chan_count,)),
            pltpu.SemaphoreType.REGULAR((chan_count,)),
        ],
        compiler_params=pltpu.CompilerParams(
            collective_id=0, has_side_effects=True, vmem_limit_bytes=58 * 1024 * 1024
        ),
    )(
        inputs, gate_logits, step_sizes.T,
        decay_rates.reshape(-1, LANES), skip_gain.reshape(-1, LANES), norm_gain.reshape(-1, LANES),
    )
    return pl.pallas_call(
        scale_kernel,
        out_shape=jax.ShapeDtypeStruct((rows, width), bf16),
        in_specs=[vmem, vmem],
        out_specs=hbm,
        scratch_shapes=[pltpu.VMEM((rows, width), bf16), dma((FINISH,))],
        compiler_params=pltpu.CompilerParams(vmem_limit_bytes=16 * 1024 * 1024),
    )(
        pltpu.with_memory_space_constraint(gated, pltpu.VMEM),
        pltpu.with_memory_space_constraint(factor, pltpu.VMEM),
    )


def solution(mesh):
    in_specs = (P("tm", "chan"), P(("tm", "chan"), None), P("tm", "chan"), P(), P(), P())
    out_specs = P(("tm", "chan"), None)
    body = functools.partial(per_device, mesh.shape["tm"], mesh.shape["chan"])
    return jax.shard_map(
        body, mesh=mesh, in_specs=in_specs, out_specs=out_specs, check_vma=False
    )
```
